512 devices in a mesh: col: 64 (over y_hi, x, z), tok: 8 (over y_lo, core).
Axes of the slice: x: 4, y: 8 (y_hi: 2, y_lo: 4; y = y_hi * 4 + y_lo), z: 8, core: 2. Of those that a mesh axis runs over, the one named last changes fastest.
Arguments:
- acts: bfloat16 [2048, 8192], P('tok', 'col'), may hold values from -6 to 6
- grad_out: bfloat16 [2048, 8192], P('tok', 'col'), may hold values from -0.19921875 to 0.19921875
- left_factor: float32 [8, 8192, 1024], P('tok', 'col'), may hold values from -6 to 6
- right_factor: float32 [8, 8192, 1024], P('tok', 'col'), may hold values from -6 to 6
- left_basis: bfloat16 [8, 8192, 1024], P('tok', 'col'), may hold values from -0.1875 to 0.1875
- right_basis: bfloat16 [8, 8192, 1024], P('tok', 'col'), may hold values from -0.1875 to 0.1875
- moment: float32 [8192, 8192], P('tok', 'col'), may hold values from -2 to 2
- second: float32 [8192, 8192], P('tok', 'col'), may hold values from 0.05 to 2
Outputs:
- left_out: float32 [8, 8192, 1024], P('tok', 'col')
- right_out: float32 [8, 8192, 1024], P('tok', 'col')
- moment_out: float32 [8192, 8192], P('tok', 'col')
- second_out: float32 [8192, 8192], P('tok', 'col')
- update: bfloat16 [8192, 8192], P('tok', 'col')
The draws below stay inside these ranges and needn't reach their ends.
All inputs are finite; a program needn't handle non-finite values.
Results may differ from the reference program's by a relative error of at most 0.0075.
Values may be sent and summed in bfloat16 or wider, within the bound.
A program may use at most 64 MiB of HBM per device.

```python
import math
import jax
import jax.numpy as jnp
from jax import lax

D = 8192
B = 1024
TOKENS = 2048


def steps_of(own_key, shape, pieces, least, largest):
    def one(dim, shards_of):
        draws = jax.random.uniform(jax.random.fold_in(jax.random.fold_in(own_key, 6), dim), (shards_of,), jnp.float32, least / len(pieces), largest / len(pieces))
        return jnp.repeat(jnp.exp(draws), shape[dim] // shards_of).reshape((-1,) + (1,) * (len(shape) - dim - 1))

    gain = one(*pieces[0])
    for cut in pieces[1:]:
        gain = gain * one(*cut)
    return gain


def scatter_about(rng, dims, scale, reach, pieces=(), held_as=jnp.bfloat16):
    array = jax.random.normal(rng, dims, jnp.float32) * scale
    if len(pieces) > 0:
        array = steps_of(rng, dims, pieces, -0.22, 0.18) * array
    return jnp.clip(array, min=-reach, max=reach).astype(held_as)


def setup_inputs(seed: int = 0) -> dict:
    seeds = jax.random.split(jax.random.key(seed), 9)
    acts = scatter_about(seeds[0], (TOKENS, D), 1.0, 6.0, ((0, 8), (1, 64)))
    grad_out = scatter_about(seeds[1], (TOKENS, D), 0.03, 0.19921875, ((0, 8), (1, 64)))
    left_factor = scatter_about(seeds[2], (D // B, D, B), 1.0, 6.0, ((0, 8), (1, 64)), jnp.float32)
    right_factor = scatter_about(seeds[3], (D // B, D, B), 1.0, 6.0, ((0, 8), (1, 64)), jnp.float32)
    left_basis = scatter_about(seeds[4], (D // B, D, B), B ** -0.5, 0.1875, ((0, 8), (1, 64)))
    right_basis = scatter_about(seeds[5], (D // B, D, B), B ** -0.5, 0.1875, ((0, 8), (1, 64)))
    moment = scatter_about(seeds[6], (D, D), 0.3, 2.0, ((0, 8), (1, 64)), jnp.float32)
    second = jnp.clip(jnp.exp(math.log(2.0) - 3.6888794 * jax.random.uniform(seeds[7], (D, D), jnp.float32) ** steps_of(seeds[7], (D, D), ((0, 8), (1, 64)), -0.2, 0.2)), 0.05, 2.0)
    return dict(acts=acts, grad_out=grad_out, left_factor=left_factor, right_factor=right_factor, left_basis=left_basis, right_basis=right_basis, moment=moment, second=second)


shampoo_beta = 0.95
first_beta = 0.9
second_beta = 0.95
first_corr = 1.0 - 0.9 ** 4
second_corr = 1.0 - 0.95 ** 4
epsilon = 1e-08

def one_block(pack):
    grads, left_fac, right_fac, left_q, right_q, first_m, second_m = pack
    left_new = shampoo_beta * left_fac + (1.0 - shampoo_beta) * jnp.dot(grads, grads.T, preferred_element_type=jnp.float32)
    right_new = shampoo_beta * right_fac + (1.0 - shampoo_beta) * jnp.dot(grads.T, grads, preferred_element_type=jnp.float32)
    mixed = jnp.dot(grads, right_q, preferred_element_type=jnp.float32).astype(jnp.bfloat16)
    rotated = jnp.dot(left_q.T, mixed, preferred_element_type=jnp.float32)
    first_new = first_beta * first_m + (1.0 - first_beta) * rotated
    second_new = second_beta * second_m + (1.0 - second_beta) * rotated * rotated
    normed = (first_new / first_corr / (jnp.sqrt(second_new / second_corr) + epsilon)).astype(jnp.bfloat16)
    back = jnp.dot(normed, right_q.T, preferred_element_type=jnp.float32).astype(jnp.bfloat16)
    update = jnp.dot(left_q, back, preferred_element_type=jnp.float32).astype(jnp.bfloat16)
    return (left_new, right_new, first_new, second_new, update)

def reference(acts, grad_out, left_factor, right_factor, left_basis, right_basis, moment, second):
    count = D // B
    grad = lax.dot_general(acts, grad_out, (((0,), (0,)), ((), ())), preferred_element_type=jnp.float32)
    tiles = grad.astype(jnp.bfloat16)

    def blockify(whole):
        return whole.reshape(count, B, count, B).transpose(0, 2, 1, 3).reshape(count * count, B, B)

    def unblock(blocked):
        return blocked.reshape(count, count, B, B).transpose(0, 2, 1, 3).reshape(D, D)

    def factored(whole):
        return whole.reshape(count * count, B, B)
    results = lax.map(one_block, (blockify(tiles), factored(left_factor), factored(right_factor), factored(left_basis), factored(right_basis), blockify(moment), blockify(second)))
    left_out = results[0].reshape(count, D, B)
    right_out = results[1].reshape(count, D, B)
    return (left_out, right_out, unblock(results[2]), unblock(results[3]), unblock(results[4]))
```

```python
import jax
import jax.numpy as jnp
from jax import lax
from jax.experimental import pallas as pl
from jax.experimental.pallas import tpu as pltpu
from jax.sharding import PartitionSpec as P

MESH = pl.DeviceIdType.MESH
F32 = jnp.float32
BF16 = jnp.bfloat16

shampoo_beta = 0.95
first_beta = 0.9
second_beta = 0.95
first_corr = 1.0 - 0.9**4
second_corr = 1.0 - 0.95**4
epsilon = 1e-08

B = 1024
W = 128
T = 256
N = 8


def dot_nn(a, b):
    return lax.dot_general(a, b, (((1,), (0,)), ((), ())), preferred_element_type=F32)


def dot_nt(a, b):
    return lax.dot_general(a, b, (((1,), (1,)), ((), ())), preferred_element_type=F32)


def lanes(k, size=W):
    return pl.ds(pl.multiple_of(k * size, size), size)


class Ring:
    def __init__(self, buf, send, recv, z, at, half):
        self.buf, self.send, self.recv, self.z, self.at, self.half = buf, send, recv, z, at, half

    @staticmethod
    def valid(s, h, way):
        return s < 3 or h == way

    def copy(self, s, h, way, slot, to):
        ref = self.buf.at[slot, self.half(h)]
        return pltpu.make_async_remote_copy(
            src_ref=ref,
            dst_ref=ref,
            send_sem=self.send.at[way, s, h],
            recv_sem=self.recv.at[way, s, h],
            device_id=self.at(to),
            device_id_type=MESH,
        )

    def outgoing(self, s, h, way):
        slot = lax.rem(self.z + (N - s if way == 0 else s), N)
        to = lax.rem(self.z + (1 if way == 0 else N - 1), N)
        return self.copy(s, h, way, slot, to)

    def incoming(self, s, h, way):
        slot = lax.rem(self.z + (N - 1 - s if way == 0 else 1 + s), N)
        to = lax.rem(self.z + (1 if way == 0 else N - 1), N)
        return self.copy(s, h, way, slot, to)

    def start(self, h):
        for way in range(2):
            self.outgoing(0, h, way).start()

    def forward(self, s, h):
        for way in range(2):
            if self.valid(s, h, way):
                self.incoming(s, h, way).wait_recv()
                if s < 3 and self.valid(s + 1, h, way):
                    self.outgoing(s + 1, h, way).start()

    def finish(self):
        for s in range(4):
            for h in range(2):
                for way in range(2):
                    if self.valid(s, h, way):
                        self.outgoing(s, h, way).wait_send()


def kernel(
    acts_in, go_in, lf_in, rf_in, ql_in, qr_in, mo_in, se_in,
    lo_out, ro_out, mo_out, se_out, up_out,
    acts_v, acts_b, at_v, go_b, psend, pown, d2d, ysend, yrecv,
    ql_b, qr_v, qrc, qrct, g_b, mixt, mo_v, se_v, lf_v, rf_v, n_b, back_v, up_v,
    load_sem, store_sem,
    ya_send, ya_recv, xa_send, xa_recv, gx_send, gx_recv, qr_send, qr_recv,
    dd_send, dd_recv, yy_send, yy_recv,
    go_rs, go_rr, ql_rs, ql_rr, g_rs, g_rr, n_rs, n_rr,
):
    tok, col = lax.axis_index("tok"), lax.axis_index("col")
    z, blk = lax.rem(col, N), lax.div(col, N)
    y_hi, x = lax.div(blk, 4), lax.rem(blk, 4)
    p, q = lax.div(tok, 4), lax.rem(tok, 4)
    a, core = lax.div(q, 2), lax.rem(q, 2)

    def dev(col_, tok_):
        return {"col": col_, "tok": tok_}

    def in_ring(z_):
        return dev(blk * N + z_, tok)

    def in_quad(p_, y_hi_):
        return dev((y_hi_ * 4 + x) * N + z, p_ * 4 + q)

    def in_row(x_):
        return dev((y_hi * 4 + x_) * N + z, tok)

    other_core = dev(col, p * 4 + a * 2 + 1 - core)
    other_y = dev(col, p * 4 + (1 - a) * 2 + core)

    def load(src, dst, n):
        c = pltpu.make_async_copy(src, dst, load_sem.at[n])
        c.start()
        return c

    go_load = load(go_in, go_b.at[z, p], 0)
    acts_load = load(acts_in, acts_v, 1)
    ql_load = [load(ql_in.at[0, pl.ds(64 * h, 64)], ql_b.at[z, h], 2 + h) for h in range(2)]
    qr_load = load(qr_in.at[0], qr_v, 4)
    late_loads = [
        load(mo_in, mo_v, 5),
        load(se_in, se_v, 6),
        load(lf_in.at[0], lf_v, 7),
        load(rf_in.at[0], rf_v, 8),
    ]

    barrier = pltpu.get_barrier_semaphore()
    partners = [in_ring(lax.rem(z + d, N)) for d in range(1, N)]
    partners += [in_row(lax.rem(x + d, 4)) for d in range(1, 4)]
    partners += [in_quad(1 - p, y_hi), in_quad(p, 1 - y_hi), in_quad(1 - p, 1 - y_hi)]
    partners += [other_core, other_y]
    for partner in partners:
        pl.semaphore_signal(barrier, inc=1, device_id=partner, device_id_type=MESH)
    pl.semaphore_wait(barrier, len(partners))

    def remote(src, dst, send, recv, to):
        return pltpu.make_async_remote_copy(
            src_ref=src, dst_ref=dst, send_sem=send, recv_sem=recv, device_id=to, device_id_type=MESH
        )

    go_ring = Ring(go_b, go_rs, go_rr, z, in_ring, lambda h: p if h == 0 else 1 - p)
    ql_ring = Ring(ql_b, ql_rs, ql_rr, z, in_ring, lambda h: h)
    g_ring = Ring(g_b, g_rs, g_rr, z, in_ring, lambda h: h)
    n_ring = Ring(n_b, n_rs, n_rr, z, in_ring, lambda h: h)

    acts_load.wait()
    home = y_hi == p

    def acts_y(d):
        return remote(acts_v, acts_b.at[x, p], ya_send.at[d], ya_recv.at[p], in_quad(y_hi, d))

    for d in range(2):
        @pl.when(jnp.logical_not(jnp.logical_and(home, y_hi == d)))
        def _():
            acts_y(d).start()

    go_load.wait()
    go_swap = remote(go_b.at[z, p], go_b.at[z, p], gx_send, gx_recv, in_quad(1 - p, y_hi))
    go_swap.start()
    go_ring.start(0)

    @pl.when(home)
    def _():
        acts_b[x, p] = acts_v[...]

    def acts_y_in(p_):
        return remote(acts_v, acts_b.at[x, p_], ya_send.at[0], ya_recv.at[p_], in_quad(p, 0))

    for p_ in range(2):
        @pl.when(jnp.logical_not(jnp.logical_and(home, p == p_)))
        def _():
            acts_y_in(p_).wait_recv()

    def acts_x(d):
        return remote(acts_b.at[x], acts_b.at[x], xa_send.at[d - 1], xa_recv.at[d - 1], in_row(lax.rem(x + d, 4)))

    def acts_x_in(d):
        slot = lax.rem(x + 4 - d, 4)
        return remote(acts_b.at[slot], acts_b.at[slot], xa_send.at[d - 1], xa_recv.at[d - 1], in_row(slot))

    for d in (2, 1, 3):
        acts_x(d).start()

    remote(go_b.at[z, 1 - p], go_b.at[z, 1 - p], gx_send, gx_recv, in_quad(1 - p, y_hi)).wait_recv()
    go_ring.start(1)
    go_ring.forward(0, 0)

    def transpose_acts(x_):
        for h in range(2):
            at_v[lax.rem(x_, 2), lax.div(x_, 2), :, h * T : (h + 1) * T] = acts_b[x_, h].T

    transpose_acts(x)
    go_ring.forward(0, 1)
    go_ring.forward(1, 0)
    acts_x_in(1).wait_recv()
    transpose_acts(lax.rem(x + 3, 4))
    go_ring.forward(1, 1)
    go_ring.forward(2, 0)
    acts_x_in(3).wait_recv()
    transpose_acts(lax.rem(x + 1, 4))
    go_ring.forward(2, 1)

    for h in range(2):
        ql_load[h].wait()
        ql_ring.start(h)
    qr_load.wait()

    def qr_out(d):
        to = lax.rem(z + d, N)
        return remote(qr_v.at[:, lanes(to)], qrc.at[z], qr_send.at[d - 1], qr_recv.at[d - 1], in_ring(to))

    def qr_incoming(d):
        slot = lax.rem(z + N - d, N)
        return remote(qrc.at[slot], qrc.at[slot], qr_send.at[d - 1], qr_recv.at[d - 1], in_ring(slot))

    for d in (4, 3, 5, 2, 6, 1, 7):
        qr_out(d).start()

    acts_x_in(2).wait_recv()
    transpose_acts(lax.rem(x + 2, 4))
    go_ring.forward(3, 0)
    go_ring.forward(3, 1)

    def partial(which, dst):
        rows = at_v[which].reshape(2 * W, 2 * T)

        @pl.loop(0, N)
        def _(k):
            dst[:, :, lanes(k)] = dot_nn(rows, go_b[k].reshape(2 * T, W)).reshape(2, W, W)

    partial(1 - core, psend)

    def to_core(a_):
        return remote(psend.at[a_], d2d.at[a_], dd_send.at[a_], dd_recv.at[a_], other_core)

    to_core(1 - a).start()
    to_core(a).start()
    partial(core, pown)
    to_core(1 - a).wait_recv()

    def to_y(h):
        return remote(ysend.at[h], yrecv.at[h], yy_send.at[h], yy_recv.at[h], other_y)

    for h in range(2):
        rows = pl.ds(64 * h, 64)
        ysend[h] = (pown[1 - a, rows] + d2d[1 - a, rows]).astype(BF16)
        to_y(h).start()
    ql_ring.forward(0, 0)
    ql_ring.forward(0, 1)
    to_core(a).wait_recv()
    pown[a] = pown[a] + d2d[a]
    for h in range(2):
        rows = pl.ds(64 * h, 64)
        to_y(h).wait_recv()
        g_b[z, h] = (pown[a, rows] + yrecv[h].astype(F32)).astype(BF16)
        g_ring.start(h)
        ql_ring.forward(1, h)

    qrc[z] = qr_v[:, lanes(z)]
    qrct[:, lanes(z)] = qrc[z].T
    for d in range(1, N):
        qr_incoming(d).wait_recv()
        slot = lax.rem(z + N - d, N)
        qrct[:, lanes(slot)] = qrc[slot].T
    ql_ring.forward(2, 0)
    ql_ring.forward(2, 1)
    g_ring.forward(0, 0)
    for c in late_loads:
        c.wait()
    rf_v[...] = shampoo_beta * rf_v[...]

    def take_tile(k):
        tile = g_b[k].reshape(W, B)
        mixt[:, lanes(k)] = dot_nt(qrct[...], tile).astype(BF16)
        own = g_b[z].reshape(W, B)
        lf_v[:, lanes(k)] = shampoo_beta * lf_v[:, lanes(k)] + (1.0 - shampoo_beta) * dot_nt(own, tile)
        part = g_b[k, :, :, lanes(z)].reshape(W, W).T
        rf_v[...] = rf_v[...] + (1.0 - shampoo_beta) * dot_nn(part, tile)

    take_tile(z)
    g_ring.forward(0, 1)
    ql_ring.forward(3, 0)
    ql_ring.forward(3, 1)
    for s in range(3):
        if s > 0:
            g_ring.forward(s, 1)
        take_tile(lax.rem(z + N - 1 - s, N))
        g_ring.forward(s + 1, 0)
        take_tile(lax.rem(z + 1 + s, N))
    g_ring.forward(3, 1)
    take_tile(lax.rem(z + 4, N))

    for h in range(2):
        for t in range(2):
            first = h * 512 + t * 256
            basis = ql_b[:, :, :, first : first + 256].reshape(B, 256)
            rotated = dot_nn(mixt[...], basis).T
            rows = pl.ds(first, 256)
            first_new = first_beta * mo_v[rows] + (1.0 - first_beta) * rotated
            second_new = second_beta * se_v[rows] + (1.0 - second_beta) * rotated * rotated
            mo_v[rows] = first_new
            se_v[rows] = second_new
            normed = first_new / first_corr / (jnp.sqrt(second_new / second_corr) + epsilon)
            n_b[z, h, t * 256 : (t + 1) * 256] = normed.astype(BF16)
        n_ring.start(h)

    def store(src, dst, n):
        c = pltpu.make_async_copy(src, dst, store_sem.at[n])
        c.start()
        return c

    stores = [
        store(lf_v, lo_out.at[0], 0),
        store(rf_v, ro_out.at[0], 1),
        store(mo_v, mo_out, 2),
        store(se_v, se_out, 3),
    ]

    def take_steps(k, h, fresh=False):
        cols = slice(h * 512, (h + 1) * 512)
        term = dot_nt(qr_v[:, lanes(k)], n_b[k, h])
        back_v[:, cols] = term if fresh else back_v[:, cols] + term

    for h in range(2):
        take_steps(z, h, True)
    for s in range(3):
        for h in range(2):
            n_ring.forward(s, h)
            take_steps(lax.rem(z + N - 1 - s, N), h)
            take_steps(lax.rem(z + 1 + s, N), h)
    for h in range(2):
        n_ring.forward(3, h)
        take_steps(lax.rem(z + 4, N), h)

    back = back_v[...].astype(BF16)
    for k in range(N):
        up_v[k * W : (k + 1) * W] = dot_nt(ql_b[k].reshape(W, B), back).astype(BF16)
    stores.append(store(up_v, up_out, 4))

    for d in range(2):
        @pl.when(jnp.logical_not(jnp.logical_and(home, y_hi == d)))
        def _():
            acts_y(d).wait_send()

    go_swap.wait_send()
    for d in range(1, 4):
        acts_x(d).wait_send()
    for d in range(1, N):
        qr_out(d).wait_send()
    for a_ in (a, 1 - a):
        to_core(a_).wait_send()
    for h in range(2):
        to_y(h).wait_send()
    for ring in (go_ring, ql_ring, g_ring, n_ring):
        ring.finish()
    for c in stores:
        c.wait()


def shards(acts, grad_out, left_factor, right_factor, left_basis, right_basis, moment, second):
    anywhere = pl.BlockSpec(memory_space=pl.ANY)
    dma, vmem = pltpu.SemaphoreType.DMA, pltpu.VMEM
    ring = [dma((2, 4, 2)), dma((2, 4, 2))]
    return pl.pallas_call(
        kernel,
        out_shape=(
            jax.ShapeDtypeStruct(left_factor.shape, F32),
            jax.ShapeDtypeStruct(right_factor.shape, F32),
            jax.ShapeDtypeStruct(moment.shape, F32),
            jax.ShapeDtypeStruct(second.shape, F32),
            jax.ShapeDtypeStruct(moment.shape, BF16),
        ),
        in_specs=[anywhere] * 8,
        out_specs=[anywhere] * 5,
        scratch_shapes=[
            vmem((T, W), BF16),
            vmem((4, 2, T, W), BF16),
            vmem((2, 2, W, 2 * T), BF16),
            vmem((N, 2, T, W), BF16),
            vmem((2, W, B), F32),
            vmem((2, W, B), F32),
            vmem((2, W, B), F32),
            vmem((2, W // 2, B), BF16),
            vmem((2, W // 2, B), BF16),
            vmem((N, 2, W // 2, B), BF16),
            vmem((W, B), BF16),
            vmem((N, W, W), BF16),
            vmem((W, B), BF16),
            vmem((N, 2, W // 2, B), BF16),
            vmem((W, B), BF16),
            vmem((B, W), F32),
            vmem((B, W), F32),
            vmem((W, B), F32),
            vmem((W, B), F32),
            vmem((N, 2, B // 2, W), BF16),
            vmem((W, B), F32),
            vmem((B, W), BF16),
            dma((9,)),
            dma((5,)),
            dma((2,)), dma((2,)),
            dma((3,)), dma((3,)),
            dma, dma,
            dma((N - 1,)), dma((N - 1,)),
            dma((2,)), dma((2,)),
            dma((2,)), dma((2,)),
            *ring, *ring, *ring, *ring,
        ],
        compiler_params=pltpu.CompilerParams(
            collective_id=0, has_side_effects=True, vmem_limit_bytes=48 * 1024 * 1024
        ),
    )(acts, grad_out, left_factor, right_factor, left_basis, right_basis, moment, second)


def solution(mesh):
    by_tile, by_rows = P("tok", "col"), P("tok", "col", None)
    return jax.shard_map(
        shards,
        mesh=mesh,
        in_specs=(by_tile, by_tile, by_rows, by_rows, by_rows, by_rows, by_tile, by_tile),
        out_specs=(by_rows, by_rows, by_tile, by_tile, by_tile),
        check_vma=False,
    )
```

```python
import jax
import jax.numpy as jnp
from jax import lax
from jax.experimental import pallas as pl
from jax.experimental.pallas import tpu as pltpu
from jax.sharding import PartitionSpec as P

MESH = pl.DeviceIdType.MESH
F32 = jnp.float32
BF16 = jnp.bfloat16

shampoo_beta = 0.95
first_beta = 0.9
second_beta = 0.95
first_corr = 1.0 - 0.9**4
second_corr = 1.0 - 0.95**4
epsilon = 1e-08

B = 1024
W = 128
T = 256
HALF = B // 2
N = 8


def dot_nn(a, b):
    return lax.dot_general(a, b, (((1,), (0,)), ((), ())), preferred_element_type=F32)


def dot_nt(a, b):
    return lax.dot_general(a, b, (((1,), (1,)), ((), ())), preferred_element_type=F32)


def lanes(k, size=W):
    return pl.ds(pl.multiple_of(k * size, size), size)


class Ring:
    def __init__(self, buf, send, recv, z, at, half):
        self.buf, self.send, self.recv, self.z, self.at, self.half = buf, send, recv, z, at, half

    @staticmethod
    def valid(s, h, way):
        return s < 3 or h == way

    def copy(self, s, h, way, slot, to):
        ref = self.buf.at[slot, self.half(h)]
        return pltpu.make_async_remote_copy(
            src_ref=ref,
            dst_ref=ref,
            send_sem=self.send.at[way, s, h],
            recv_sem=self.recv.at[way, s, h],
            device_id=self.at(to),
            device_id_type=MESH,
        )

    def outgoing(self, s, h, way):
        slot = lax.rem(self.z + (N - s if way == 0 else s), N)
        to = lax.rem(self.z + (1 if way == 0 else N - 1), N)
        return self.copy(s, h, way, slot, to)

    def incoming(self, s, h, way):
        slot = lax.rem(self.z + (N - 1 - s if way == 0 else 1 + s), N)
        to = lax.rem(self.z + (1 if way == 0 else N - 1), N)
        return self.copy(s, h, way, slot, to)

    def start(self, h):
        for way in range(2):
            self.outgoing(0, h, way).start()

    def forward(self, s, h):
        for way in range(2):
            if self.valid(s, h, way):
                self.incoming(s, h, way).wait_recv()
                if s < 3 and self.valid(s + 1, h, way):
                    self.outgoing(s + 1, h, way).start()

    def finish(self):
        for s in range(4):
            for h in range(2):
                for way in range(2):
                    if self.valid(s, h, way):
                        self.outgoing(s, h, way).wait_send()


def kernel(
    acts_in, go_in, lf_in, rf_in, ql_in, qr_in, mo_in, se_in,
    lf_v, rf_v, mo_v, se_v, back_v, ql_b,
    acts_v, acts_b, at_v, go_b, psend, pown, d2d, ysend, yrecv,
    qr_v, qrc, qrct, g_b, mixt, n_b, sums,
    load_sem,
    ya_send, ya_recv, xa_send, xa_recv, gx_send, gx_recv, qr_send, qr_recv,
    dd_send, dd_recv, yy_send, yy_recv,
    go_rs, go_rr, ql_rs, ql_rr, g_rs, g_rr, n_rs, n_rr,
):
    tok, col = lax.axis_index("tok"), lax.axis_index("col")
    z, blk = lax.rem(col, N), lax.div(col, N)
    y_hi, x = lax.div(blk, 4), lax.rem(blk, 4)
    p, q = lax.div(tok, 4), lax.rem(tok, 4)
    a, core = lax.div(q, 2), lax.rem(q, 2)

    def dev(col_, tok_):
        return {"col": col_, "tok": tok_}

    def in_ring(z_):
        return dev(blk * N + z_, tok)

    def in_quad(p_, y_hi_):
        return dev((y_hi_ * 4 + x) * N + z, p_ * 4 + q)

    def in_row(x_):
        return dev((y_hi * 4 + x_) * N + z, tok)

    other_core = dev(col, p * 4 + a * 2 + 1 - core)
    other_y = dev(col, p * 4 + (1 - a) * 2 + core)

    def load(src, dst, n):
        c = pltpu.make_async_copy(src, dst, load_sem.at[n])
        c.start()
        return c

    go_load = load(go_in, go_b.at[z, p], 0)
    acts_load = load(acts_in, acts_v, 1)
    ql_load = [load(ql_in.at[0, :, pl.ds(HALF * h, HALF)], ql_b.at[z, h], 2 + h) for h in range(2)]
    qr_load = load(qr_in.at[0], qr_v, 4)
    late_loads = [
        load(mo_in, mo_v, 5),
        load(se_in, se_v, 6),
        load(lf_in.at[0], lf_v, 7),
        load(rf_in.at[0], rf_v, 8),
    ]

    barrier = pltpu.get_barrier_semaphore()
    partners = [in_ring(lax.rem(z + d, N)) for d in range(1, N)]
    partners += [in_row(lax.rem(x + d, 4)) for d in range(1, 4)]
    partners += [in_quad(1 - p, y_hi), in_quad(p, 1 - y_hi), in_quad(1 - p, 1 - y_hi)]
    partners += [other_core, other_y]
    for partner in partners:
        pl.semaphore_signal(barrier, inc=1, device_id=partner, device_id_type=MESH)
    pl.semaphore_wait(barrier, len(partners))

    def remote(src, dst, send, recv, to):
        return pltpu.make_async_remote_copy(
            src_ref=src, dst_ref=dst, send_sem=send, recv_sem=recv, device_id=to, device_id_type=MESH
        )

    go_ring = Ring(go_b, go_rs, go_rr, z, in_ring, lambda h: p if h == 0 else 1 - p)
    ql_ring = Ring(ql_b, ql_rs, ql_rr, z, in_ring, lambda h: h)
    g_ring = Ring(g_b, g_rs, g_rr, z, in_ring, lambda h: h)
    n_ring = Ring(n_b, n_rs, n_rr, z, in_ring, lambda h: h)

    go_load.wait()
    go_ring.start(0)
    go_swap = remote(go_b.at[z, p], go_b.at[z, p], gx_send, gx_recv, in_quad(1 - p, y_hi))
    go_swap.start()

    acts_load.wait()
    home = y_hi == p

    def acts_y(d):
        return remote(acts_v, acts_b.at[x, p], ya_send.at[d], ya_recv.at[p], in_quad(y_hi, d))

    for d in range(2):
        @pl.when(jnp.logical_not(jnp.logical_and(home, y_hi == d)))
        def _():
            acts_y(d).start()

    ql_load[0].wait()
    ql_ring.start(0)

    @pl.when(home)
    def _():
        acts_b[x, p] = acts_v[...]

    remote(go_b.at[z, 1 - p], go_b.at[z, 1 - p], gx_send, gx_recv, in_quad(1 - p, y_hi)).wait_recv()
    go_ring.start(1)
    go_ring.forward(0, 0)

    def acts_y_in(p_):
        return remote(acts_v, acts_b.at[x, p_], ya_send.at[0], ya_recv.at[p_], in_quad(p, 0))

    for p_ in range(2):
        @pl.when(jnp.logical_not(jnp.logical_and(home, p == p_)))
        def _():
            acts_y_in(p_).wait_recv()

    def acts_x(d):
        return remote(acts_b.at[x], acts_b.at[x], xa_send.at[d - 1], xa_recv.at[d - 1], in_row(lax.rem(x + d, 4)))

    def acts_x_in(d):
        slot = lax.rem(x + 4 - d, 4)
        return remote(acts_b.at[slot], acts_b.at[slot], xa_send.at[d - 1], xa_recv.at[d - 1], in_row(slot))

    for d in (2, 1, 3):
        acts_x(d).start()

    qr_load.wait()

    def qr_out(d):
        to = lax.rem(z + d, N)
        return remote(qr_v.at[:, lanes(to)], qrc.at[z], qr_send.at[d - 1], qr_recv.at[d - 1], in_ring(to))

    def qr_incoming(d):
        slot = lax.rem(z + N - d, N)
        return remote(qrc.at[slot], qrc.at[slot], qr_send.at[d - 1], qr_recv.at[d - 1], in_ring(slot))

    def transpose_acts(x_):
        for h in range(2):
            at_v[lax.rem(x_, 2), lax.div(x_, 2), :, h * T : (h + 1) * T] = acts_b[x_, h].T

    for d in (4, 3, 5):
        qr_out(d).start()
    go_ring.forward(0, 1)
    go_ring.forward(1, 0)
    transpose_acts(x)
    ql_ring.forward(0, 0)
    go_ring.forward(1, 1)
    for d in (2, 6, 1, 7):
        qr_out(d).start()
    go_ring.forward(2, 0)
    acts_x_in(1).wait_recv()
    transpose_acts(lax.rem(x + 3, 4))
    go_ring.forward(2, 1)
    acts_x_in(3).wait_recv()
    transpose_acts(lax.rem(x + 1, 4))
    acts_x_in(2).wait_recv()
    transpose_acts(lax.rem(x + 2, 4))

    def chunk(place):
        ahead, step = lax.rem(place, 2), lax.div(place + 1, 2)
        return lax.rem(z + ahead * step + (1 - ahead) * (N - step), N)

    groups = (slice(0, 5), slice(5, 8))

    def partial(group):
        @pl.loop(group.start, group.stop)
        def _(place):
            part = go_b[chunk(place)].reshape(2 * T, W)
            psend[:, place] = dot_nn(at_v[1 - core].reshape(2 * W, 2 * T), part).reshape(2, W, W)
            pown[:, place] = dot_nn(at_v[core].reshape(2 * W, 2 * T), part).reshape(2, W, W)

    def to_core(n, a_):
        span = pl.ds(groups[n].start, groups[n].stop - groups[n].start)
        return remote(psend.at[a_, span], d2d.at[a_, span], dd_send.at[n, a_], dd_recv.at[n, a_], other_core)

    def to_y(n):
        span = pl.ds(groups[n].start, groups[n].stop - groups[n].start)
        return remote(ysend.at[span], yrecv.at[span], yy_send.at[n], yy_recv.at[n], other_y)

    def send_y(n):
        to_core(n, 1 - a).wait_recv()
        for place in range(groups[n].start, groups[n].stop):
            ysend[place] = (pown[1 - a, place] + d2d[1 - a, place]).astype(BF16)
        to_y(n).start()

    def take_y(n):
        to_core(n, a).wait_recv()
        to_y(n).wait_recv()
        for place in range(groups[n].start, groups[n].stop):
            tile = (pown[a, place] + d2d[a, place] + yrecv[place].astype(F32)).astype(BF16)
            g_b[z, :, :, lanes(chunk(place))] = tile.reshape(2, W // 2, W)

    partial(groups[0])
    to_core(0, 1 - a).start()
    to_core(0, a).start()
    go_ring.forward(3, 0)
    go_ring.forward(3, 1)
    ql_ring.forward(1, 0)
    partial(groups[1])
    to_core(1, 1 - a).start()
    to_core(1, a).start()
    send_y(0)
    send_y(1)
    ql_ring.forward(2, 0)

    qrc[z] = qr_v[:, lanes(z)]
    qrct[:, lanes(z)] = qrc[z].T
    for d in range(1, N):
        qr_incoming(d).wait_recv()
        slot = lax.rem(z + N - d, N)
        qrct[:, lanes(slot)] = qrc[slot].T

    take_y(0)
    take_y(1)
    for h in range(2):
        g_ring.start(h)

    def mix(k):
        mixt[:, lanes(k)] = dot_nt(qrct[...], g_b[k].reshape(W, B)).astype(BF16)

    mix(z)
    ql_ring.forward(3, 0)
    for s in range(3):
        g_ring.forward(s, 0)
        g_ring.forward(s, 1)
        if s == 0:
            ql_load[1].wait()
            ql_ring.start(1)
        else:
            ql_ring.forward(s - 1, 1)
        mix(lax.rem(z + N - 1 - s, N))
        mix(lax.rem(z + 1 + s, N))
    g_ring.forward(3, 0)
    g_ring.forward(3, 1)
    mix(lax.rem(z + 4, N))
    for c in late_loads:
        c.wait()

    def rotate(h):
        for t in range(2):
            basis = ql_b[:, h, :, t * 256 : (t + 1) * 256].reshape(B, 256)
            rotated = dot_nn(mixt[...], basis).T
            rows = pl.ds(h * HALF + t * 256, 256)
            first_new = first_beta * mo_v[rows] + (1.0 - first_beta) * rotated
            second_new = second_beta * se_v[rows] + (1.0 - second_beta) * rotated * rotated
            mo_v[rows] = first_new
            se_v[rows] = second_new
            normed = first_new / first_corr / (jnp.sqrt(second_new / second_corr) + epsilon)
            n_b[z, h, t * 256 : (t + 1) * 256] = normed.astype(BF16)
        n_ring.start(h)

    def factors(k):
        tile = g_b[k].reshape(W, B)
        lf_v[:, lanes(k)] = shampoo_beta * lf_v[:, lanes(k)] + (1.0 - shampoo_beta) * dot_nt(g_b[z].reshape(W, B), tile)
        part = g_b[k, :, :, lanes(z)].reshape(W, W).T
        rf_v[...] = rf_v[...] + (1.0 - shampoo_beta) * dot_nn(part, tile)

    def take_steps(k, h, fresh=False):
        cols = slice(h * HALF, (h + 1) * HALF)
        term = dot_nt(qr_v[:, lanes(k)], n_b[k, h])
        sums[:, cols] = term if fresh else sums[:, cols] + term

    rotate(0)
    ql_ring.forward(2, 1)
    rf_v[...] = shampoo_beta * rf_v[...]
    take_steps(z, 0, True)
    ql_ring.forward(3, 1)
    rotate(1)
    take_steps(z, 1, True)
    for s in range(3):
        for h in range(2):
            n_ring.forward(s, h)
            take_steps(lax.rem(z + N - 1 - s, N), h)
            take_steps(lax.rem(z + 1 + s, N), h)
            factors(lax.rem(z + 2 * s + h, N))
    factors(lax.rem(z + 6, N))
    factors(lax.rem(z + 7, N))
    for h in range(2):
        n_ring.forward(3, h)
        take_steps(lax.rem(z + 4, N), h)
    back_v[...] = sums[...].astype(BF16)

    for d in range(2):
        @pl.when(jnp.logical_not(jnp.logical_and(home, y_hi == d)))
        def _():
            acts_y(d).wait_send()

    go_swap.wait_send()
    for d in range(1, 4):
        acts_x(d).wait_send()
    for d in range(1, N):
        qr_out(d).wait_send()
    for n in range(2):
        for a_ in (a, 1 - a):
            to_core(n, a_).wait_send()
        to_y(n).wait_send()
    for ring in (go_ring, ql_ring, g_ring, n_ring):
        ring.finish()


def finish(lf_v, rf_v, mo_v, se_v, back_v, ql_b, lo_out, ro_out, mo_out, se_out, up_out, up_v, store_sem):
    def store(src, dst, n):
        c = pltpu.make_async_copy(src, dst, store_sem.at[n])
        c.start()
        return c

    stores = [
        store(lf_v, lo_out.at[0], 0),
        store(rf_v, ro_out.at[0], 1),
        store(mo_v, mo_out, 2),
        store(se_v, se_out, 3),
    ]
    for k in range(N):
        total = dot_nt(ql_b[k, 0], back_v[:, :HALF]) + dot_nt(ql_b[k, 1], back_v[:, HALF:])
        up_v[k * W : (k + 1) * W] = total.astype(BF16)
    stores.append(store(up_v, up_out, 4))
    for c in stores:
        c.wait()


def shards(acts, grad_out, left_factor, right_factor, left_basis, right_basis, moment, second):
    dma, vmem = pltpu.SemaphoreType.DMA, pltpu.VMEM
    hbm, on_chip = pl.BlockSpec(memory_space=pltpu.HBM), pl.BlockSpec(memory_space=pltpu.VMEM)
    ring = [dma((2, 4, 2)), dma((2, 4, 2))]
    arrays = (acts, grad_out, left_factor, right_factor, left_basis, right_basis, moment, second)
    shape = jax.ShapeDtypeStruct
    held = pl.pallas_call(
        kernel,
        out_shape=(
            shape((W, B), F32),
            shape((W, B), F32),
            shape((B, W), F32),
            shape((B, W), F32),
            shape((W, B), BF16),
            shape((N, 2, W, HALF), BF16),
        ),
        in_specs=[hbm] * 8,
        out_specs=[on_chip] * 6,
        scratch_shapes=[
            vmem((T, W), BF16),
            vmem((4, 2, T, W), BF16),
            vmem((2, 2, W, 2 * T), BF16),
            vmem((N, 2, T, W), BF16),
            vmem((2, N, W, W), F32),
            vmem((2, N, W, W), F32),
            vmem((2, N, W, W), F32),
            vmem((N, W, W), BF16),
            vmem((N, W, W), BF16),
            vmem((W, B), BF16),
            vmem((N, W, W), BF16),
            vmem((W, B), BF16),
            vmem((N, 2, W // 2, B), BF16),
            vmem((W, B), BF16),
            vmem((N, 2, HALF, W), BF16),
            vmem((W, B), F32),
            dma((9,)),
            dma((2,)), dma((2,)),
            dma((3,)), dma((3,)),
            dma, dma,
            dma((N - 1,)), dma((N - 1,)),
            dma((2, 2)), dma((2, 2)),
            dma((2,)), dma((2,)),
            *ring, *ring, *ring, *ring,
        ],
        compiler_params=pltpu.CompilerParams(
            collective_id=0, has_side_effects=True, vmem_limit_bytes=40 * 1024 * 1024
        ),
    )(*(pltpu.with_memory_space_constraint(v, pltpu.HBM) for v in arrays))
    return pl.pallas_call(
        finish,
        out_shape=(
            shape(left_factor.shape, F32),
            shape(right_factor.shape, F32),
            shape(moment.shape, F32),
            shape(second.shape, F32),
            shape(moment.shape, BF16),
        ),
        in_specs=[on_chip] * 6,
        out_specs=[hbm] * 5,
        scratch_shapes=[vmem((B, W), BF16), dma((5,))],
        compiler_params=pltpu.CompilerParams(vmem_limit_bytes=16 * 1024 * 1024),
    )(*held)


def solution(mesh):
    by_tile, by_rows = P("tok", "col"), P("tok", "col", None)
    return jax.shard_map(
        shards,
        mesh=mesh,
        in_specs=(by_tile, by_tile, by_rows, by_rows, by_rows, by_rows, by_tile, by_tile),
        out_specs=(by_rows, by_rows, by_tile, by_tile, by_tile),
        check_vma=False,
    )
```

```python
import jax
import jax.numpy as jnp
from jax import lax
from jax.experimental import pallas as pl
from jax.experimental.pallas import tpu as pltpu
from jax.sharding import PartitionSpec as P

MESH = pl.DeviceIdType.MESH
F32 = jnp.float32
BF16 = jnp.bfloat16

shampoo_beta = 0.95
first_beta = 0.9
second_beta = 0.95
first_corr = 1.0 - 0.9**4
second_corr = 1.0 - 0.95**4
epsilon = 1e-08

B = 1024
W = 128
T = 256
HALF = B // 2
N = 8


def dot_nn(a, b):
    return lax.dot_general(a, b, (((1,), (0,)), ((), ())), preferred_element_type=F32)


def dot_nt(a, b):
    return lax.dot_general(a, b, (((1,), (1,)), ((), ())), preferred_element_type=F32)


def lanes(k, size=W):
    return pl.ds(pl.multiple_of(k * size, size), size)


class Ring:
    def __init__(self, buf, send, recv, z, at, place=lambda h: h):
        self.buf, self.send, self.recv, self.z, self.at, self.place = buf, send, recv, z, at, place
        self.pieces = buf.shape[1]

    def ways(self, s, h):
        return (0, 1) if s < 3 else (0,) if 2 * h < self.pieces else (1,)

    def copy(self, s, h, way, slot, to):
        ref = self.buf.at[slot, self.place(h)]
        return pltpu.make_async_remote_copy(
            src_ref=ref,
            dst_ref=ref,
            send_sem=self.send.at[way, s, h],
            recv_sem=self.recv.at[way, s, h],
            device_id=self.at(to),
            device_id_type=MESH,
        )

    def outgoing(self, s, h, way):
        slot = lax.rem(self.z + (N - s if way == 0 else s), N)
        to = lax.rem(self.z + (1 if way == 0 else N - 1), N)
        return self.copy(s, h, way, slot, to)

    def incoming(self, s, h, way):
        slot = lax.rem(self.z + (N - 1 - s if way == 0 else 1 + s), N)
        to = lax.rem(self.z + (1 if way == 0 else N - 1), N)
        return self.copy(s, h, way, slot, to)

    def start(self, h):
        for way in (0, 1):
            self.outgoing(0, h, way).start()

    def forward(self, s, h):
        for way in self.ways(s, h):
            self.incoming(s, h, way).wait_recv()
            if s < 3 and way in self.ways(s + 1, h):
                self.outgoing(s + 1, h, way).start()

    def finish(self):
        for s in range(4):
            for h in range(self.pieces):
                for way in self.ways(s, h):
                    self.outgoing(s, h, way).wait_send()


def kernel(
    acts_in, go_in, lf_in, rf_in, ql_in, qr_in, mo_in, se_in,
    lf_v, rf_v, mo_v, se_v, back_v, ql_b,
    acts_v, relay, acts_b, at_v, go_b, psend, pown, d2d, ysend, yrecv,
    qr_v, qrc, qrct, g_b, mixt, n_b, sums,
    load_sem,
    ya_send, ya_recv, xa_send, xa_recv, gx_send, gx_recv, qr_send, qr_recv,
    dd_send, dd_recv, yy_send, yy_recv,
    go_rs, go_rr, ql_rs, ql_rr, g_rs, g_rr, n_rs, n_rr,
):
    tok, col = lax.axis_index("tok"), lax.axis_index("col")
    z, blk = lax.rem(col, N), lax.div(col, N)
    y_hi, x = lax.div(blk, 4), lax.rem(blk, 4)
    p, q = lax.div(tok, 4), lax.rem(tok, 4)
    a, core = lax.div(q, 2), lax.rem(q, 2)

    def dev(col_, tok_):
        return {"col": col_, "tok": tok_}

    def in_ring(z_):
        return dev(blk * N + z_, tok)

    def in_quad(p_, y_hi_):
        return dev((y_hi_ * 4 + x) * N + z, p_ * 4 + q)

    def in_row(x_):
        return dev((y_hi * 4 + x_) * N + z, tok)

    other_core = dev(col, p * 4 + a * 2 + 1 - core)
    other_y = dev(col, p * 4 + (1 - a) * 2 + core)

    def load(src, dst, n):
        c = pltpu.make_async_copy(src, dst, load_sem.at[n])
        c.start()
        return c

    go_load = load(go_in, go_b.at[z, p], 0)
    acts_load = load(acts_in, acts_v, 1)
    ql_load = [load(ql_in.at[0, :, pl.ds(HALF * h, HALF)], ql_b.at[z, h], 2 + h) for h in range(2)]
    qr_load = load(qr_in.at[0], qr_v, 4)
    late_loads = [
        load(mo_in, mo_v, 5),
        load(se_in, se_v, 6),
        load(lf_in.at[0], lf_v, 7),
        load(rf_in.at[0], rf_v, 8),
    ]

    barrier = pltpu.get_barrier_semaphore()
    partners = [in_ring(lax.rem(z + d, N)) for d in range(1, N)]
    partners += [in_row(lax.rem(x + d, 4)) for d in range(1, 4)]
    partners += [in_quad(1 - p, y_hi), in_quad(p, 1 - y_hi), in_quad(1 - p, 1 - y_hi)]
    partners += [other_core, other_y]
    for partner in partners:
        pl.semaphore_signal(barrier, inc=1, device_id=partner, device_id_type=MESH)
    pl.semaphore_wait(barrier, len(partners))

    def remote(src, dst, send, recv, to):
        return pltpu.make_async_remote_copy(
            src_ref=src, dst_ref=dst, send_sem=send, recv_sem=recv, device_id=to, device_id_type=MESH
        )

    go_ring = Ring(go_b, go_rs, go_rr, z, in_ring, lambda h: p if h == 0 else 1 - p)
    ql_ring = Ring(ql_b, ql_rs, ql_rr, z, in_ring)
    g_ring = Ring(g_b, g_rs, g_rr, z, in_ring)
    n_ring = Ring(n_b, n_rs, n_rr, z, in_ring)

    go_load.wait()
    go_ring.start(0)
    go_swap = remote(go_b.at[z, p], go_b.at[z, p], gx_send, gx_recv, in_quad(1 - p, y_hi))
    go_swap.start()

    acts_load.wait()
    home = y_hi == p
    last = jnp.logical_and(p == 1, y_hi == 1)
    third = jnp.logical_and(p == 0, y_hi == 1)

    def acts_y(d):
        return remote(acts_v, acts_b.at[x, p], ya_send.at[d], ya_recv.at[p], in_quad(y_hi, d))

    def acts_back():
        return remote(acts_v, relay, ya_send.at[0], ya_recv.at[2], in_quad(0, 1))

    def acts_relay():
        return remote(relay, acts_b.at[x, 1], ya_send.at[2], ya_recv.at[1], in_quad(1, 0))

    def direct(d):
        same = jnp.logical_and(home, y_hi == d)
        return jnp.logical_not(jnp.logical_or(same, last) if d == 0 else same)

    for d in range(2):
        @pl.when(direct(d))
        def _():
            acts_y(d).start()

    @pl.when(last)
    def _():
        acts_back().start()

    qr_load.wait()

    def qr_out(d):
        to = lax.rem(z + d, N)
        return remote(qr_v.at[:, lanes(to)], qrc.at[z], qr_send.at[d - 1], qr_recv.at[d - 1], in_ring(to))

    def qr_incoming(d):
        slot = lax.rem(z + N - d, N)
        return remote(qrc.at[slot], qrc.at[slot], qr_send.at[d - 1], qr_recv.at[d - 1], in_ring(slot))

    ql_load[0].wait()
    ql_ring.start(0)

    @pl.when(home)
    def _():
        acts_b[x, p] = acts_v[...]

    def acts_y_in(p_):
        return remote(acts_v, acts_b.at[x, p_], ya_send.at[0], ya_recv.at[p_], in_quad(p, 0))

    right, left = lax.rem(x + 1, 4), lax.rem(x + 3, 4)

    def acts_x(n, kind, x_, to):
        ref = acts_b.at[x_, y_hi if n == 0 else 1 - y_hi]
        return remote(ref, ref, xa_send.at[n, kind], xa_recv.at[n, kind], in_row(to))

    def acts_x_out(n, kind):
        if kind < 2:
            return acts_x(n, kind, x, (right, left)[kind])
        return acts_x(n, 2, left, right) if n == 0 else acts_x(n, 2, right, left)

    def acts_x_slot(kind):
        return (left, right, lax.rem(x + 2, 4))[kind]

    def acts_x_in(n, kind):
        return acts_x(n, kind, acts_x_slot(kind), right)

    def transpose_acts(n, x_):
        p_ = y_hi if n == 0 else 1 - y_hi
        at_v[lax.rem(x_, 2), lax.div(x_, 2), :, lanes(p_, T)] = acts_b[x_, p_].T

    @pl.when(jnp.logical_not(home))
    def _():
        acts_y_in(y_hi).wait_recv()

    for kind in range(2):
        acts_x_out(0, kind).start()
    go_ring.forward(0, 0)
    remote(go_b.at[z, 1 - p], go_b.at[z, 1 - p], gx_send, gx_recv, in_quad(1 - p, y_hi)).wait_recv()
    go_ring.start(1)

    @pl.when(third)
    def _():
        acts_back().wait_recv()
        acts_relay().start()

    acts_x_in(0, 0).wait_recv()
    acts_x_out(0, 2).start()
    go_ring.forward(1, 0)
    ql_ring.forward(0, 0)
    acts_y_in(1 - y_hi).wait_recv()
    for kind in range(2):
        acts_x_out(1, kind).start()
    go_ring.forward(0, 1)
    for n in range(2):
        transpose_acts(n, x)
    transpose_acts(0, left)
    acts_x_in(0, 1).wait_recv()
    transpose_acts(0, right)
    go_ring.forward(2, 0)
    acts_x_in(1, 1).wait_recv()
    acts_x_out(1, 2).start()
    go_ring.forward(1, 1)
    ql_ring.forward(1, 0)
    ql_load[1].wait()
    ql_ring.start(1)
    transpose_acts(1, right)
    acts_x_in(1, 0).wait_recv()
    transpose_acts(1, left)
    for n in range(2):
        acts_x_in(n, 2).wait_recv()
        transpose_acts(n, acts_x_slot(2))
    go_ring.forward(3, 0)

    def chunk(place):
        ahead, step = lax.rem(place, 2), lax.div(place + 1, 2)
        return lax.rem(z + ahead * step + (1 - ahead) * (N - step), N)

    groups = (slice(0, 5), slice(5, 7), slice(7, 8))

    def span(n):
        return pl.ds(groups[n].start, groups[n].stop - groups[n].start)

    def partial(n):
        @pl.loop(groups[n].start, groups[n].stop)
        def _(place):
            part = go_b[chunk(place)].reshape(2 * T, W)
            psend[:, place] = dot_nn(at_v[1 - core].reshape(2 * W, 2 * T), part).reshape(2, W, W)
            pown[:, place] = dot_nn(at_v[core].reshape(2 * W, 2 * T), part).reshape(2, W, W)

        for a_ in (1 - a, a):
            to_core(n, a_).start()

    def to_core(n, a_):
        return remote(psend.at[a_, span(n)], d2d.at[a_, span(n)], dd_send.at[n, a_], dd_recv.at[n, a_], other_core)

    def to_y(n):
        return remote(ysend.at[span(n)], yrecv.at[span(n)], yy_send.at[n], yy_recv.at[n], other_y)

    def send_y(n):
        to_core(n, 1 - a).wait_recv()
        for place in range(groups[n].start, groups[n].stop):
            ysend[place] = (pown[1 - a, place] + d2d[1 - a, place]).astype(BF16)
        to_y(n).start()

    def take_y(n):
        to_core(n, a).wait_recv()
        to_y(n).wait_recv()
        for place in range(groups[n].start, groups[n].stop):
            tile = (pown[a, place] + d2d[a, place] + yrecv[place].astype(F32)).astype(BF16)
            g_b[z, :, :, lanes(chunk(place))] = tile.reshape(4, W // 4, W)

    partial(0)
    go_ring.forward(2, 1)
    ql_ring.forward(2, 0)
    partial(1)
    send_y(0)
    for d in (1, 7, 2, 6):
        qr_out(d).start()
    ql_ring.forward(0, 1)
    go_ring.forward(3, 1)
    partial(2)
    send_y(1)
    send_y(2)
    for d in (3, 5, 4):
        qr_out(d).start()
    ql_ring.forward(3, 0)
    ql_ring.forward(1, 1)
    for n in range(3):
        take_y(n)
    for h in range(4):
        g_ring.start(h)

    qrc[z] = qr_v[:, lanes(z)]
    qrct[:, lanes(z)] = qrc[z].T
    for d in range(1, N):
        qr_incoming(d).wait_recv()
        slot = lax.rem(z + N - d, N)
        qrct[:, lanes(slot)] = qrc[slot].T

    def mix(k):
        mixt[:, lanes(k)] = dot_nt(qrct[...], g_b[k].reshape(W, B)).astype(BF16)

    mix(z)
    for s in range(3):
        for h in range(4):
            g_ring.forward(s, h)
        if s < 2:
            ql_ring.forward(2 + s, 1)
        mix(lax.rem(z + N - 1 - s, N))
        mix(lax.rem(z + 1 + s, N))
    for h in range(4):
        g_ring.forward(3, h)
    mix(lax.rem(z + 4, N))
    for c in late_loads:
        c.wait()

    def rotate(h):
        basis = ql_b[:, h // 2, :, (h % 2) * 256 : (h % 2 + 1) * 256].reshape(B, 256)
        rotated = dot_nn(mixt[...], basis).T
        rows = pl.ds(h * 256, 256)
        first_new = first_beta * mo_v[rows] + (1.0 - first_beta) * rotated
        second_new = second_beta * se_v[rows] + (1.0 - second_beta) * rotated * rotated
        mo_v[rows] = first_new
        se_v[rows] = second_new
        normed = first_new / first_corr / (jnp.sqrt(second_new / second_corr) + epsilon)
        n_b[z, h] = normed.astype(BF16)
        n_ring.start(h)

    def factors(k):
        tile = g_b[k].reshape(W, B)
        lf_v[:, lanes(k)] = shampoo_beta * lf_v[:, lanes(k)] + (1.0 - shampoo_beta) * dot_nt(g_b[z].reshape(W, B), tile)
        part = g_b[k, :, :, lanes(z)].reshape(W, W).T
        rf_v[...] = rf_v[...] + (1.0 - shampoo_beta) * dot_nn(part, tile)

    def take_steps(k, h, fresh=False):
        cols = slice(h * 256, (h + 1) * 256)
        term = dot_nt(qr_v[:, lanes(k)], n_b[k, h])
        sums[:, cols] = term if fresh else sums[:, cols] + term

    for h in range(4):
        rotate(h)
    rf_v[...] = shampoo_beta * rf_v[...]
    for h in range(4):
        take_steps(z, h, True)
    for s in range(3):
        for h in range(4):
            n_ring.forward(s, h)
            take_steps(lax.rem(z + N - 1 - s, N), h)
            take_steps(lax.rem(z + 1 + s, N), h)
            if h % 2 == 1:
                factors(lax.rem(z + 2 * s + h // 2, N))
    factors(lax.rem(z + 6, N))
    factors(lax.rem(z + 7, N))
    for h in range(4):
        n_ring.forward(3, h)
        take_steps(lax.rem(z + 4, N), h)
    back_v[...] = sums[...].astype(BF16)

    for d in range(2):
        @pl.when(direct(d))
        def _():
            acts_y(d).wait_send()

    @pl.when(last)
    def _():
        acts_back().wait_send()

    @pl.when(third)
    def _():
        acts_relay().wait_send()

    go_swap.wait_send()
    for n in range(2):
        for kind in range(3):
            acts_x_out(n, kind).wait_send()
    for d in range(1, N):
        qr_out(d).wait_send()
    for n in range(3):
        for a_ in (a, 1 - a):
            to_core(n, a_).wait_send()
        to_y(n).wait_send()
    for ring in (go_ring, ql_ring, g_ring, n_ring):
        ring.finish()


def finish(lf_v, rf_v, mo_v, se_v, back_v, ql_b, lo_out, ro_out, mo_out, se_out, up_out, up_v, store_sem):
    def store(src, dst, n):
        c = pltpu.make_async_copy(src, dst, store_sem.at[n])
        c.start()
        return c

    stores = [
        store(lf_v, lo_out.at[0], 0),
        store(rf_v, ro_out.at[0], 1),
        store(mo_v, mo_out, 2),
        store(se_v, se_out, 3),
    ]
    for k in range(N):
        total = dot_nt(ql_b[k, 0], back_v[:, :HALF]) + dot_nt(ql_b[k, 1], back_v[:, HALF:])
        up_v[k * W : (k + 1) * W] = total.astype(BF16)
    stores.append(store(up_v, up_out, 4))
    for c in stores:
        c.wait()


def shards(acts, grad_out, left_factor, right_factor, left_basis, right_basis, moment, second):
    dma, vmem = pltpu.SemaphoreType.DMA, pltpu.VMEM
    hbm, on_chip = pl.BlockSpec(memory_space=pltpu.HBM), pl.BlockSpec(memory_space=pltpu.VMEM)
    halves, quarters = [dma((2, 4, 2))] * 2, [dma((2, 4, 4))] * 2
    arrays = (acts, grad_out, left_factor, right_factor, left_basis, right_basis, moment, second)
    shape = jax.ShapeDtypeStruct
    held = pl.pallas_call(
        kernel,
        out_shape=(
            shape((W, B), F32),
            shape((W, B), F32),
            shape((B, W), F32),
            shape((B, W), F32),
            shape((W, B), BF16),
            shape((N, 2, W, HALF), BF16),
        ),
        in_specs=[hbm] * 8,
        out_specs=[on_chip] * 6,
        scratch_shapes=[
            vmem((T, W), BF16),
            vmem((T, W), BF16),
            vmem((4, 2, T, W), BF16),
            vmem((2, 2, W, 2 * T), BF16),
            vmem((N, 2, T, W), BF16),
            vmem((2, N, W, W), F32),
            vmem((2, N, W, W), F32),
            vmem((2, N, W, W), F32),
            vmem((N, W, W), BF16),
            vmem((N, W, W), BF16),
            vmem((W, B), BF16),
            vmem((N, W, W), BF16),
            vmem((W, B), BF16),
            vmem((N, 4, W // 4, B), BF16),
            vmem((W, B), BF16),
            vmem((N, 4, 256, W), BF16),
            vmem((W, B), F32),
            dma((9,)),
            dma((3,)), dma((3,)),
            dma((2, 3)), dma((2, 3)),
            dma, dma,
            dma((N - 1,)), dma((N - 1,)),
            dma((3, 2)), dma((3, 2)),
            dma((3,)), dma((3,)),
            *halves, *halves, *quarters, *quarters,
        ],
        compiler_params=pltpu.CompilerParams(
            collective_id=0, has_side_effects=True, vmem_limit_bytes=40 * 1024 * 1024
        ),
    )(*(pltpu.with_memory_space_constraint(v, pltpu.HBM) for v in arrays))
    return pl.pallas_call(
        finish,
        out_shape=(
            shape(left_factor.shape, F32),
            shape(right_factor.shape, F32),
            shape(moment.shape, F32),
            shape(second.shape, F32),
            shape(moment.shape, BF16),
        ),
        in_specs=[on_chip] * 6,
        out_specs=[hbm] * 5,
        scratch_shapes=[vmem((B, W), BF16), dma((5,))],
        compiler_params=pltpu.CompilerParams(vmem_limit_bytes=16 * 1024 * 1024),
    )(*held)


def solution(mesh):
    by_tile, by_rows = P("tok", "col"), P("tok", "col", None)
    return jax.shard_map(
        shards,
        mesh=mesh,
        in_specs=(by_tile, by_tile, by_rows, by_rows, by_rows, by_rows, by_tile, by_tile),
        out_specs=(by_rows, by_rows, by_tile, by_tile, by_tile),
        check_vma=False,
    )
```

```python
import jax
import jax.numpy as jnp
from jax import lax
from jax.experimental import pallas as pl
from jax.experimental.pallas import tpu as pltpu
from jax.sharding import PartitionSpec as P

MESH = pl.DeviceIdType.MESH
F32 = jnp.float32
BF16 = jnp.bfloat16

shampoo_beta = 0.95
first_beta = 0.9
second_beta = 0.95
first_corr = 1.0 - 0.9**4
second_corr = 1.0 - 0.95**4
epsilon = 1e-08

B = 1024
W = 128
T = 256
HALF = B // 2
N = 8


def dot_nn(a, b):
    return lax.dot_general(a, b, (((1,), (0,)), ((), ())), preferred_element_type=F32)


def dot_nt(a, b):
    return lax.dot_general(a, b, (((1,), (1,)), ((), ())), preferred_element_type=F32)


def lanes(k, size=W):
    return pl.ds(pl.multiple_of(k * size, size), size)


class Ring:
    def __init__(self, buf, send, recv, z, at, place=lambda h: h):
        self.buf, self.send, self.recv, self.z, self.at, self.place = buf, send, recv, z, at, place
        self.pieces = buf.shape[1]

    def ways(self, s, h):
        return (0, 1) if s < 3 else (0,) if 2 * h < self.pieces else (1,)

    def copy(self, s, h, way, slot, to):
        ref = self.buf.at[slot, self.place(h)]
        return pltpu.make_async_remote_copy(
            src_ref=ref,
            dst_ref=ref,
            send_sem=self.send.at[way, s, h],
            recv_sem=self.recv.at[way, s, h],
            device_id=self.at(to),
            device_id_type=MESH,
        )

    def outgoing(self, s, h, way):
        slot = lax.rem(self.z + (N - s if way == 0 else s), N)
        to = lax.rem(self.z + (1 if way == 0 else N - 1), N)
        return self.copy(s, h, way, slot, to)

    def incoming(self, s, h, way):
        slot = lax.rem(self.z + (N - 1 - s if way == 0 else 1 + s), N)
        to = lax.rem(self.z + (1 if way == 0 else N - 1), N)
        return self.copy(s, h, way, slot, to)

    def start(self, h):
        for way in (0, 1):
            self.outgoing(0, h, way).start()

    def forward(self, s, h):
        for way in self.ways(s, h):
            self.incoming(s, h, way).wait_recv()
            if s < 3 and way in self.ways(s + 1, h):
                self.outgoing(s + 1, h, way).start()

    def finish(self):
        for s in range(4):
            for h in range(self.pieces):
                for way in self.ways(s, h):
                    self.outgoing(s, h, way).wait_send()


def kernel(
    acts_in, go_in, lf_in, rf_in, ql_in, qr_in, mo_in, se_in,
    lf_v, rf_v, mo_v, se_v, back_v, ql_b,
    acts_v, relay, acts_b, at_v, go_b, psend, pown, d2d, ysend, yrecv,
    qr_v, qrc, qrct, g_b, mixt, n_b, sums,
    load_sem,
    ya_send, ya_recv, xa_send, xa_recv, gx_send, gx_recv, qr_send, qr_recv,
    dd_send, dd_recv, yy_send, yy_recv,
    go_rs, go_rr, ql_rs, ql_rr, g_rs, g_rr, n_rs, n_rr,
):
    tok, col = lax.axis_index("tok"), lax.axis_index("col")
    z, blk = lax.rem(col, N), lax.div(col, N)
    y_hi, x = lax.div(blk, 4), lax.rem(blk, 4)
    p, q = lax.div(tok, 4), lax.rem(tok, 4)
    a, core = lax.div(q, 2), lax.rem(q, 2)

    def dev(col_, tok_):
        return {"col": col_, "tok": tok_}

    def in_ring(z_):
        return dev(blk * N + z_, tok)

    def in_quad(p_, y_hi_):
        return dev((y_hi_ * 4 + x) * N + z, p_ * 4 + q)

    def in_row(x_):
        return dev((y_hi * 4 + x_) * N + z, tok)

    other_core = dev(col, p * 4 + a * 2 + 1 - core)
    other_y = dev(col, p * 4 + (1 - a) * 2 + core)

    def load(src, dst, n):
        c = pltpu.make_async_copy(src, dst, load_sem.at[n])
        c.start()
        return c

    go_load = load(go_in, go_b.at[z, p], 0)
    acts_load = load(acts_in, acts_v, 1)
    ql_load = [load(ql_in.at[0, :, pl.ds(HALF * h, HALF)], ql_b.at[z, h], 2 + h) for h in range(2)]
    qr_load = load(qr_in.at[0], qr_v, 4)
    late_loads = [
        load(mo_in, mo_v, 5),
        load(se_in, se_v, 6),
        load(lf_in.at[0], lf_v, 7),
        load(rf_in.at[0], rf_v, 8),
    ]

    barrier = pltpu.get_barrier_semaphore()
    partners = [in_ring(lax.rem(z + d, N)) for d in range(1, N)]
    partners += [in_row(lax.rem(x + d, 4)) for d in range(1, 4)]
    partners += [in_quad(1 - p, y_hi), in_quad(p, 1 - y_hi), in_quad(1 - p, 1 - y_hi)]
    partners += [other_core, other_y]
    for partner in partners:
        pl.semaphore_signal(barrier, inc=1, device_id=partner, device_id_type=MESH)
    pl.semaphore_wait(barrier, len(partners))

    def remote(src, dst, send, recv, to):
        return pltpu.make_async_remote_copy(
            src_ref=src, dst_ref=dst, send_sem=send, recv_sem=recv, device_id=to, device_id_type=MESH
        )

    go_ring = Ring(go_b, go_rs, go_rr, z, in_ring, lambda h: p if h == 0 else 1 - p)
    ql_ring = Ring(ql_b, ql_rs, ql_rr, z, in_ring)
    g_ring = Ring(g_b, g_rs, g_rr, z, in_ring)
    n_ring = Ring(n_b, n_rs, n_rr, z, in_ring)

    go_load.wait()
    go_ring.start(0)
    go_swap = remote(go_b.at[z, p], go_b.at[z, p], gx_send, gx_recv, in_quad(1 - p, y_hi))
    go_swap.start()

    acts_load.wait()
    home = y_hi == p
    last = jnp.logical_and(p == 1, y_hi == 1)
    third = jnp.logical_and(p == 0, y_hi == 1)

    def acts_y(d):
        return remote(acts_v, acts_b.at[x, p], ya_send.at[d], ya_recv.at[p], in_quad(y_hi, d))

    def acts_back():
        return remote(acts_v, relay, ya_send.at[0], ya_recv.at[2], in_quad(0, 1))

    def acts_relay():
        return remote(relay, acts_b.at[x, 1], ya_send.at[2], ya_recv.at[1], in_quad(1, 0))

    def direct(d):
        same = jnp.logical_and(home, y_hi == d)
        return jnp.logical_not(jnp.logical_or(same, last) if d == 0 else same)

    for d in range(2):
        @pl.when(direct(d))
        def _():
            acts_y(d).start()

    @pl.when(last)
    def _():
        acts_back().start()

    qr_load.wait()

    def qr_out(d):
        to = lax.rem(z + d, N)
        return remote(qr_v.at[:, lanes(to)], qrc.at[z], qr_send.at[d - 1], qr_recv.at[d - 1], in_ring(to))

    def qr_incoming(d):
        slot = lax.rem(z + N - d, N)
        return remote(qrc.at[slot], qrc.at[slot], qr_send.at[d - 1], qr_recv.at[d - 1], in_ring(slot))

    ql_load[0].wait()
    ql_ring.start(0)

    @pl.when(home)
    def _():
        acts_b[x, p] = acts_v[...]

    def acts_y_in(p_):
        return remote(acts_v, acts_b.at[x, p_], ya_send.at[0], ya_recv.at[p_], in_quad(p, 0))

    right, left = lax.rem(x + 1, 4), lax.rem(x + 3, 4)

    def acts_x(n, kind, x_, to):
        ref = acts_b.at[x_, y_hi if n == 0 else 1 - y_hi]
        return remote(ref, ref, xa_send.at[n, kind], xa_recv.at[n, kind], in_row(to))

    def acts_x_out(n, kind):
        if kind < 2:
            return acts_x(n, kind, x, (right, left)[kind])
        return acts_x(n, 2, left, right) if n == 0 else acts_x(n, 2, right, left)

    def acts_x_slot(kind):
        return (left, right, lax.rem(x + 2, 4))[kind]

    def acts_x_in(n, kind):
        return acts_x(n, kind, acts_x_slot(kind), right)

    def transpose_acts(n, x_):
        p_ = y_hi if n == 0 else 1 - y_hi
        at_v[lax.rem(x_, 2), lax.div(x_, 2), :, lanes(p_, T)] = acts_b[x_, p_].T

    @pl.when(jnp.logical_not(home))
    def _():
        acts_y_in(y_hi).wait_recv()

    for kind in range(2):
        acts_x_out(0, kind).start()
    go_ring.forward(0, 0)
    remote(go_b.at[z, 1 - p], go_b.at[z, 1 - p], gx_send, gx_recv, in_quad(1 - p, y_hi)).wait_recv()
    go_ring.start(1)

    @pl.when(third)
    def _():
        acts_back().wait_recv()
        acts_relay().start()

    acts_x_in(0, 0).wait_recv()
    acts_x_out(0, 2).start()
    go_ring.forward(1, 0)
    ql_ring.forward(0, 0)
    acts_y_in(1 - y_hi).wait_recv()
    for kind in range(2):
        acts_x_out(1, kind).start()
    go_ring.forward(0, 1)
    for n in range(2):
        transpose_acts(n, x)
    transpose_acts(0, left)
    acts_x_in(0, 1).wait_recv()
    transpose_acts(0, right)
    go_ring.forward(2, 0)
    acts_x_in(1, 1).wait_recv()
    acts_x_out(1, 2).start()
    go_ring.forward(1, 1)
    ql_ring.forward(1, 0)
    ql_load[1].wait()
    ql_ring.start(1)
    transpose_acts(1, right)
    acts_x_in(1, 0).wait_recv()
    transpose_acts(1, left)
    for n in range(2):
        acts_x_in(n, 2).wait_recv()
        transpose_acts(n, acts_x_slot(2))
    go_ring.forward(3, 0)

    def chunk(place):
        ahead, step = lax.rem(place, 2), lax.div(place + 1, 2)
        return lax.rem(z + ahead * step + (1 - ahead) * (N - step), N)

    groups = (slice(0, 5), slice(5, 7), slice(7, 8))

    def span(n):
        return pl.ds(groups[n].start, groups[n].stop - groups[n].start)

    def partial(n):
        @pl.loop(groups[n].start, groups[n].stop)
        def _(place):
            part = go_b[chunk(place)].reshape(2 * T, W)
            psend[:, place] = dot_nn(at_v[1 - core].reshape(2 * W, 2 * T), part).reshape(2, W, W)
            pown[:, place] = dot_nn(at_v[core].reshape(2 * W, 2 * T), part).reshape(2, W, W)

        for a_ in (1 - a, a):
            to_core(n, a_).start()

    def to_core(n, a_):
        return remote(psend.at[a_, span(n)], d2d.at[a_, span(n)], dd_send.at[n, a_], dd_recv.at[n, a_], other_core)

    def to_y(n):
        return remote(ysend.at[span(n)], yrecv.at[span(n)], yy_send.at[n], yy_recv.at[n], other_y)

    def send_y(n):
        to_core(n, 1 - a).wait_recv()
        for place in range(groups[n].start, groups[n].stop):
            ysend[place] = (pown[1 - a, place] + d2d[1 - a, place]).astype(BF16)
        to_y(n).start()

    def take_y(n):
        to_core(n, a).wait_recv()
        to_y(n).wait_recv()
        for place in range(groups[n].start, groups[n].stop):
            tile = (pown[a, place] + d2d[a, place] + yrecv[place].astype(F32)).astype(BF16)
            g_b[z, :, :, lanes(chunk(place))] = tile.reshape(4, W // 4, W)

    partial(0)
    go_ring.forward(2, 1)
    ql_ring.forward(2, 0)
    partial(1)
    send_y(0)
    for d in (1, 7, 2, 6):
        qr_out(d).start()
    ql_ring.forward(0, 1)
    go_ring.forward(3, 1)
    partial(2)
    send_y(1)
    send_y(2)
    for d in (3, 5, 4):
        qr_out(d).start()
    ql_ring.forward(3, 0)
    ql_ring.forward(1, 1)
    for n in range(3):
        take_y(n)
    for h in range(4):
        g_ring.start(h)

    qrc[z] = qr_v[:, lanes(z)]
    qrct[:, lanes(z)] = qrc[z].T
    for d in range(1, N):
        qr_incoming(d).wait_recv()
        slot = lax.rem(z + N - d, N)
        qrct[:, lanes(slot)] = qrc[slot].T

    def mix(k):
        mixt[:, lanes(k)] = dot_nt(qrct[...], g_b[k].reshape(W, B)).astype(BF16)

    mix(z)
    for s in range(3):
        for h in range(4):
            g_ring.forward(s, h)
        if s == 1:
            ql_ring.forward(2, 1)
        mix(lax.rem(z + N - 1 - s, N))
        mix(lax.rem(z + 1 + s, N))
    for h in range(4):
        g_ring.forward(3, h)
    mix(lax.rem(z + 4, N))
    for c in late_loads:
        c.wait()

    def rotate(h):
        basis = ql_b[:, h // 2, :, (h % 2) * 256 : (h % 2 + 1) * 256].reshape(B, 256)
        rotated = dot_nn(mixt[...], basis).T
        rows = pl.ds(h * 256, 256)
        first_new = first_beta * mo_v[rows] + (1.0 - first_beta) * rotated
        second_new = second_beta * se_v[rows] + (1.0 - second_beta) * rotated * rotated
        mo_v[rows] = first_new
        se_v[rows] = second_new
        normed = first_new / first_corr / (jnp.sqrt(second_new / second_corr) + epsilon)
        n_b[z, h] = normed.astype(BF16)
        n_ring.start(h)

    def factors(k):
        tile = g_b[k].reshape(W, B)
        lf_v[:, lanes(k)] = shampoo_beta * lf_v[:, lanes(k)] + (1.0 - shampoo_beta) * dot_nt(g_b[z].reshape(W, B), tile)
        part = g_b[k, :, :, lanes(z)].reshape(W, W).T
        rf_v[...] = rf_v[...] + (1.0 - shampoo_beta) * dot_nn(part, tile)

    def take_steps(k, h, fresh=False):
        cols = slice(h * 256, (h + 1) * 256)
        term = dot_nt(qr_v[:, lanes(k)], n_b[k, h])
        sums[:, cols] = term if fresh else sums[:, cols] + term

    for h in range(4):
        if h == 2:
            ql_ring.forward(3, 1)
        rotate(h)
    rf_v[...] = shampoo_beta * rf_v[...]
    for h in range(4):
        take_steps(z, h, True)
    for s in range(3):
        for h in range(4):
            n_ring.forward(s, h)
            take_steps(lax.rem(z + N - 1 - s, N), h)
            take_steps(lax.rem(z + 1 + s, N), h)
            if h % 2 == 1:
                factors(lax.rem(z + 2 * s + h // 2, N))
    factors(lax.rem(z + 6, N))
    factors(lax.rem(z + 7, N))
    for h in range(4):
        n_ring.forward(3, h)
        take_steps(lax.rem(z + 4, N), h)
    back_v[...] = sums[...].astype(BF16)

    for d in range(2):
        @pl.when(direct(d))
        def _():
            acts_y(d).wait_send()

    @pl.when(last)
    def _():
        acts_back().wait_send()

    @pl.when(third)
    def _():
        acts_relay().wait_send()

    go_swap.wait_send()
    for n in range(2):
        for kind in range(3):
            acts_x_out(n, kind).wait_send()
    for d in range(1, N):
        qr_out(d).wait_send()
    for n in range(3):
        for a_ in (a, 1 - a):
            to_core(n, a_).wait_send()
        to_y(n).wait_send()
    for ring in (go_ring, ql_ring, g_ring, n_ring):
        ring.finish()


def finish(lf_v, rf_v, mo_v, se_v, back_v, ql_b, lo_out, ro_out, mo_out, se_out, up_out, up_v, store_sem):
    def store(src, dst, n):
        c = pltpu.make_async_copy(src, dst, store_sem.at[n])
        c.start()
        return c

    stores = [
        store(lf_v, lo_out.at[0], 0),
        store(rf_v, ro_out.at[0], 1),
        store(mo_v, mo_out, 2),
        store(se_v, se_out, 3),
    ]
    for k in range(N):
        total = dot_nt(ql_b[k, 0], back_v[:, :HALF]) + dot_nt(ql_b[k, 1], back_v[:, HALF:])
        up_v[k * W : (k + 1) * W] = total.astype(BF16)
    stores.append(store(up_v, up_out, 4))
    for c in stores:
        c.wait()


def shards(acts, grad_out, left_factor, right_factor, left_basis, right_basis, moment, second):
    dma, vmem = pltpu.SemaphoreType.DMA, pltpu.VMEM
    hbm, on_chip = pl.BlockSpec(memory_space=pltpu.HBM), pl.BlockSpec(memory_space=pltpu.VMEM)
    halves, quarters = [dma((2, 4, 2))] * 2, [dma((2, 4, 4))] * 2
    arrays = (acts, grad_out, left_factor, right_factor, left_basis, right_basis, moment, second)
    shape = jax.ShapeDtypeStruct
    held = pl.pallas_call(
        kernel,
        out_shape=(
            shape((W, B), F32),
            shape((W, B), F32),
            shape((B, W), F32),
            shape((B, W), F32),
            shape((W, B), BF16),
            shape((N, 2, W, HALF), BF16),
        ),
        in_specs=[hbm] * 8,
        out_specs=[on_chip] * 6,
        scratch_shapes=[
            vmem((T, W), BF16),
            vmem((T, W), BF16),
            vmem((4, 2, T, W), BF16),
            vmem((2, 2, W, 2 * T), BF16),
            vmem((N, 2, T, W), BF16),
            vmem((2, N, W, W), F32),
            vmem((2, N, W, W), F32),
            vmem((2, N, W, W), F32),
            vmem((N, W, W), BF16),
            vmem((N, W, W), BF16),
            vmem((W, B), BF16),
            vmem((N, W, W), BF16),
            vmem((W, B), BF16),
            vmem((N, 4, W // 4, B), BF16),
            vmem((W, B), BF16),
            vmem((N, 4, 256, W), BF16),
            vmem((W, B), F32),
            dma((9,)),
            dma((3,)), dma((3,)),
            dma((2, 3)), dma((2, 3)),
            dma, dma,
            dma((N - 1,)), dma((N - 1,)),
            dma((3, 2)), dma((3, 2)),
            dma((3,)), dma((3,)),
            *halves, *halves, *quarters, *quarters,
        ],
        compiler_params=pltpu.CompilerParams(
            collective_id=0, has_side_effects=True, vmem_limit_bytes=40 * 1024 * 1024
        ),
    )(*(pltpu.with_memory_space_constraint(v, pltpu.HBM) for v in arrays))
    return pl.pallas_call(
        finish,
        out_shape=(
            shape(left_factor.shape, F32),
            shape(right_factor.shape, F32),
            shape(moment.shape, F32),
            shape(second.shape, F32),
            shape(moment.shape, BF16),
        ),
        in_specs=[on_chip] * 6,
        out_specs=[hbm] * 5,
        scratch_shapes=[vmem((B, W), BF16), dma((5,))],
        compiler_params=pltpu.CompilerParams(vmem_limit_bytes=16 * 1024 * 1024),
    )(*held)


def solution(mesh):
    by_tile, by_rows = P("tok", "col"), P("tok", "col", None)
    return jax.shard_map(
        shards,
        mesh=mesh,
        in_specs=(by_tile, by_tile, by_rows, by_rows, by_rows, by_rows, by_tile, by_tile),
        out_specs=(by_rows, by_rows, by_tile, by_tile, by_tile),
        check_vma=False,
    )
```
